32 devices in a mesh: tp: 4 (over z), fsdp: 8 (over y, x, core).
Axes of the slice: x: 2, y: 2, z: 4, core: 2. Of those that a mesh axis runs over, the one named last changes fastest.
Arguments:
- img: bfloat16 [64, 128, 1536], P('fsdp')
- txt: bfloat16 [64, 128, 1536], P('fsdp')
- vec: bfloat16 [64, 1536], P('fsdp')
- ids: int32 [64, 256, 3], P('fsdp')
- d_img: bfloat16 [64, 128, 1536], P('fsdp')
- d_txt: bfloat16 [64, 128, 1536], P('fsdp')
- w_mod: bfloat16 [2, 1536, 6, 1536], P(None, 'fsdp', None, 'tp')
- b_mod: bfloat16 [2, 6, 1536], P(None, None, 'tp')
- w_qkv: bfloat16 [2, 1536, 3, 1536], P(None, 'fsdp', None, 'tp')
- b_qkv: bfloat16 [2, 3, 1536], P(None, None, 'tp')
- qk_gain: bfloat16 [2, 2, 64], replicated
- w_proj: bfloat16 [2, 1536, 1536], P(None, ('tp', 'fsdp'))
- b_proj: bfloat16 [2, 1536], replicated
- w_fc1: bfloat16 [2, 1536, 6144], P(None, 'fsdp', 'tp')
- b_fc1: bfloat16 [2, 6144], P(None, 'tp')
- w_fc2: bfloat16 [2, 6144, 1536], P(None, ('tp', 'fsdp'))
- b_fc2: bfloat16 [2, 1536], replicated
Outputs:
- output 1: bfloat16 [64, 128, 1536], P('fsdp')
- output 2: bfloat16 [64, 128, 1536], P('fsdp')
- output 3: bfloat16 [64, 128, 1536], P('fsdp')
- output 4: bfloat16 [64, 128, 1536], P('fsdp')
- output 5: float32 [64, 1536], P('fsdp')
- output 6: float32 [2, 1536, 6, 1536], P(None, 'fsdp', None, 'tp')
- output 7: float32 [2, 6, 1536], P(None, None, 'tp')
- output 8: float32 [2, 1536, 3, 1536], P(None, 'fsdp', None, 'tp')
- output 9: float32 [2, 3, 1536], P(None, None, 'tp')
- output 10: float32 [2, 2, 64], replicated
- output 11: float32 [2, 1536, 1536], P(None, ('tp', 'fsdp'))
- output 12: float32 [2, 1536], replicated
- output 13: float32 [2, 1536, 6144], P(None, 'fsdp', 'tp')
- output 14: float32 [2, 6144], P(None, 'tp')
- output 15: float32 [2, 6144, 1536], P(None, ('tp', 'fsdp'))
- output 16: float32 [2, 1536], replicated
All inputs are finite; a program needn't handle non-finite values.
Results may differ from the reference program's by a relative error of at most 0.0127138.
Values are sent between devices in bfloat16 or wider.
A program may use at most 1 GiB of HBM per device.

```python
import jax
import jax.numpy as jnp
from jax import lax

D = 1536
HEADS = 24
HEAD = 64
FF = 6144
BATCH = 64
TXT = 128
IMG = 128
TP = 4
FSDP = 8

WIDTH = HEADS * HEAD
TOKENS = TXT + IMG
ROPE_FIRST = HEAD // 8
ROPE_REST = (HEAD - ROPE_FIRST) // 2
NORM_EPS = 1e-6
ROPE_THETA = 10000.0


def setup_inputs(seed: int = 0) -> dict:
    keys = jax.random.split(jax.random.key(seed), 17)

    def draw(key_index, shape, spread):
        return jax.random.normal(keys[key_index], shape, jnp.float32) * spread

    return {
        'img': draw(0, (BATCH, IMG, D), 1.0).astype(jnp.bfloat16),
        'txt': draw(1, (BATCH, TXT, D), 1.0).astype(jnp.bfloat16),
        'vec': draw(2, (BATCH, D), 1.0).astype(jnp.bfloat16),
        'ids': jax.random.randint(keys[3], (BATCH, TOKENS, 3), 0, 64, jnp.int32),
        'd_img': draw(4, (BATCH, IMG, D), 1.0).astype(jnp.bfloat16),
        'd_txt': draw(5, (BATCH, TXT, D), 1.0).astype(jnp.bfloat16),
        'w_mod': draw(6, (2, D, 6, D), D ** -0.5).astype(jnp.bfloat16),
        'b_mod': draw(7, (2, 6, D), 0.3).astype(jnp.bfloat16),
        'w_qkv': draw(8, (2, D, 3, WIDTH), D ** -0.5).astype(jnp.bfloat16),
        'b_qkv': draw(9, (2, 3, WIDTH), 0.3).astype(jnp.bfloat16),
        'qk_gain': (1.0 + draw(10, (2, 2, HEAD), 0.3)).astype(jnp.bfloat16),
        'w_proj': draw(11, (2, WIDTH, D), WIDTH ** -0.5).astype(jnp.bfloat16),
        'b_proj': draw(12, (2, D), 0.3).astype(jnp.bfloat16),
        'w_fc1': draw(13, (2, D, FF), D ** -0.5).astype(jnp.bfloat16),
        'b_fc1': draw(14, (2, FF), 0.3).astype(jnp.bfloat16),
        'w_fc2': draw(15, (2, FF, D), FF ** -0.5).astype(jnp.bfloat16),
        'b_fc2': draw(16, (2, D), 0.3).astype(jnp.bfloat16),
    }


def layer_norm(values):
    centered = values - jnp.mean(values, -1, keepdims=True)
    return centered * lax.rsqrt(jnp.mean(jnp.square(centered), -1, keepdims=True) + NORM_EPS)


def modulate(values, shift, scale):
    return (layer_norm(values) * (1.0 + scale[:, None, :]) + shift[:, None, :]).astype(jnp.bfloat16)


def rms_norm(values):
    return values * lax.rsqrt(jnp.mean(jnp.square(values), -1, keepdims=True) + NORM_EPS)


def rope_tables(ids):
    angles = []
    for axis, width in enumerate((ROPE_FIRST, ROPE_REST, ROPE_REST)):
        omega = ROPE_THETA ** (-jnp.arange(0, width, 2, dtype=jnp.float32) / width)
        angles.append(ids[:, :, axis:axis + 1].astype(jnp.float32) * omega)
    angle = jnp.concatenate(angles, -1)
    return jnp.cos(angle), jnp.sin(angle)


def apply_rope(values, cosine, sine):
    pairs = values.reshape(values.shape[:-1] + (values.shape[-1] // 2, 2))
    even = pairs[..., 0]
    odd = pairs[..., 1]
    cos_rows = cosine[:, :, None, :]
    sin_rows = sine[:, :, None, :]
    return jnp.stack([cos_rows * even - sin_rows * odd, sin_rows * even + cos_rows * odd], -1).reshape(values.shape)


def qk_prep(qkv_raw, gain, cosine, sine):
    shape4 = qkv_raw.shape[:2] + (HEADS, HEAD)
    query = rms_norm(qkv_raw[:, :, 0].reshape(shape4)) * gain[0]
    key_vals = rms_norm(qkv_raw[:, :, 1].reshape(shape4)) * gain[1]
    value = qkv_raw[:, :, 2].reshape(shape4).astype(jnp.bfloat16)
    return (apply_rope(query, cosine, sine).astype(jnp.bfloat16), apply_rope(key_vals, cosine, sine).astype(jnp.bfloat16), value)


def attend_one(operands):
    query, key_vals, value = operands
    scores = jnp.einsum('qhd,khd->hqk', query.astype(jnp.float32), key_vals.astype(jnp.float32)) * HEAD ** -0.5
    probs = jax.nn.softmax(scores, -1).astype(jnp.bfloat16)
    return jnp.einsum('hqk,khd->qhd', probs.astype(jnp.float32), value.astype(jnp.float32)).astype(jnp.bfloat16)


def grouped_product(act, weight):
    act4 = act.reshape(act.shape[0], act.shape[1], TP, -1).astype(jnp.float32)
    weight3 = weight.reshape(TP, -1, weight.shape[-1])
    part = jnp.einsum('bltk,tkd->bltd', act4, weight3).astype(jnp.bfloat16)
    return jnp.sum(part.astype(jnp.float32), 2)


def block(img, txt, vec_f32, ids, weights):
    w_mod, b_mod, w_qkv, b_qkv, qk_gain, w_proj, b_proj, w_fc1, b_fc1, w_fc2, b_fc2 = weights
    silu_vec = jax.nn.silu(vec_f32).astype(jnp.bfloat16).astype(jnp.float32)
    cosine, sine = rope_tables(ids)
    branches = (txt, img)
    spans = ((0, TXT), (TXT, TOKENS))
    modul_list = []
    joint_parts = ([], [], [])
    for branch in range(2):
        begin, end = spans[branch]
        modul = jnp.einsum('bd,dke->bke', silu_vec, w_mod[branch]) + b_mod[branch]
        normed = modulate(branches[branch].astype(jnp.float32), modul[:, 0], modul[:, 1])
        qkv_raw = jnp.einsum('bld,dke->blke', normed.astype(jnp.float32), w_qkv[branch]) + b_qkv[branch]
        prepared = qk_prep(qkv_raw, qk_gain[branch], cosine[:, begin:end], sine[:, begin:end])
        for index in range(3):
            joint_parts[index].append(prepared[index])
        modul_list.append(modul)
    joint = tuple(jnp.concatenate(parts, 1) for parts in joint_parts)
    attn = lax.map(jax.checkpoint(attend_one), joint).reshape(BATCH, TOKENS, WIDTH)
    outputs = []
    for branch in range(2):
        begin, end = spans[branch]
        modul = modul_list[branch]
        resid_in = branches[branch].astype(jnp.float32)
        attn_proj = grouped_product(attn[:, begin:end], w_proj[branch]) + b_proj[branch]
        resid_mid = resid_in + modul[:, 2, None, :] * attn_proj
        normed = modulate(resid_mid, modul[:, 3], modul[:, 4])
        pre_act = jnp.einsum('bld,df->blf', normed.astype(jnp.float32), w_fc1[branch]) + b_fc1[branch]
        hidden = jax.nn.gelu(pre_act, approximate=True).astype(jnp.bfloat16)
        mlp_out = grouped_product(hidden, w_fc2[branch]) + b_fc2[branch]
        outputs.append((resid_mid + modul[:, 5, None, :] * mlp_out).astype(jnp.bfloat16))
    return outputs[1], outputs[0]


def reference(img, txt, vec, ids, d_img, d_txt, w_mod, b_mod, w_qkv, b_qkv, qk_gain, w_proj, b_proj, w_fc1, b_fc1, w_fc2, b_fc2):
    weights = tuple(weight.astype(jnp.float32) for weight in (w_mod, b_mod, w_qkv, b_qkv, qk_gain, w_proj, b_proj, w_fc1, b_fc1, w_fc2, b_fc2))

    def forward(img_in, txt_in, vec_in, weight_set):
        return block(img_in, txt_in, vec_in, ids, weight_set)

    outputs, pullback = jax.vjp(forward, img, txt, vec.astype(jnp.float32), weights)
    g_img, g_txt, g_vec, g_weights = pullback((d_img, d_txt))
    grads = tuple(grad_sum / FSDP for grad_sum in g_weights)
    return (outputs[0], outputs[1], g_img, g_txt, g_vec, grads[0], grads[1], grads[2], grads[3], grads[4], grads[5], grads[6], grads[7], grads[8], grads[9], grads[10])
```

```python
import functools
import jax
import jax.numpy as jnp
from jax import lax
from jax.sharding import PartitionSpec as P

NORM_EPS = 1e-6
ROPE_THETA = 10000.0
BF16 = jnp.bfloat16
F32 = jnp.float32


def layer_norm(values):
    centered = values - jnp.mean(values, -1, keepdims=True)
    return centered * lax.rsqrt(jnp.mean(jnp.square(centered), -1, keepdims=True) + NORM_EPS)


def modulate(values, shift, scale):
    return (layer_norm(values) * (1.0 + scale[:, None, :]) + shift[:, None, :]).astype(BF16)


def rms_norm(values):
    return values * lax.rsqrt(jnp.mean(jnp.square(values), -1, keepdims=True) + NORM_EPS)


def rope_tables(ids, head_dim):
    first = head_dim // 8
    rest = (head_dim - first) // 2
    angles = []
    for axis, width in enumerate((first, rest, rest)):
        omega = ROPE_THETA ** (-jnp.arange(0, width, 2, dtype=F32) / width)
        angles.append(ids[:, :, axis:axis + 1].astype(F32) * omega)
    angle = jnp.concatenate(angles, -1)
    return jnp.cos(angle), jnp.sin(angle)


def apply_rope(values, cosine, sine):
    pairs = values.reshape(values.shape[:-1] + (values.shape[-1] // 2, 2))
    even = pairs[..., 0]
    odd = pairs[..., 1]
    cos_rows = cosine[:, :, None, :]
    sin_rows = sine[:, :, None, :]
    return jnp.stack([cos_rows * even - sin_rows * odd, sin_rows * even + cos_rows * odd], -1).reshape(values.shape)


def qk_prep(qkv_raw, gain, cosine, sine):
    head_dim = gain.shape[-1]
    shape4 = qkv_raw.shape[:2] + (qkv_raw.shape[3] // head_dim, head_dim)
    query = rms_norm(qkv_raw[:, :, 0].reshape(shape4)) * gain[0]
    key_vals = rms_norm(qkv_raw[:, :, 1].reshape(shape4)) * gain[1]
    value = qkv_raw[:, :, 2].reshape(shape4).astype(BF16)
    return (apply_rope(query, cosine, sine).astype(BF16), apply_rope(key_vals, cosine, sine).astype(BF16), value)


def attend(query, key_vals, value):
    scores = jnp.einsum('bqhd,bkhd->bhqk', query, key_vals, preferred_element_type=F32) * query.shape[-1] ** -0.5
    probs = jax.nn.softmax(scores, -1).astype(BF16)
    return jnp.einsum('bhqk,bkhd->bqhd', probs, value, preferred_element_type=F32).astype(BF16)


def gelu_bf16(pre_act):
    return jax.nn.gelu(pre_act, approximate=True).astype(BF16)


def silu_bf16(vec_f32):
    return jax.nn.silu(vec_f32).astype(BF16)


def mm(spec, a, b):
    return jnp.einsum(spec, a, b, preferred_element_type=F32)


def solution(mesh):
    n_tp = mesh.shape['tp']
    n_fsdp = mesh.shape['fsdp']
    grad_scale = 1.0 / n_fsdp
    act_spec = P('fsdp', None, None)
    vec_spec = P('fsdp', None)
    weight_specs = (P(None, 'fsdp', None, 'tp'), P(None, None, 'tp'), P(None, 'fsdp', None, 'tp'), P(None, None, 'tp'), P(), P(None, ('tp', 'fsdp'), None), P(), P(None, 'fsdp', 'tp'), P(None, 'tp'), P(None, ('tp', 'fsdp'), None), P())
    in_specs = (act_spec, act_spec, vec_spec, act_spec, act_spec, act_spec) + weight_specs
    out_specs = (act_spec, act_spec, act_spec, act_spec, vec_spec) + weight_specs

    def shift(x, k):
        return lax.ppermute(x, 'tp', [(i, (i + k) % n_tp) for i in range(n_tp)])

    def line_gather(own, z):
        right, left = [own], [own]
        for t in range(1, n_tp):
            right.append(lax.ppermute(right[-1], 'tp', [(i, i + 1) for i in range(t - 1, n_tp - 1)]))
            left.append(lax.ppermute(left[-1], 'tp', [(i, i - 1) for i in range(1, n_tp - t + 1)]))
        return [own] + [jnp.where(z + k < n_tp, left[k], right[n_tp - k]) for k in range(1, n_tp)]

    def line_scatter(slots):
        right = left = None
        for t in range(1, n_tp):
            r, l = slots[n_tp - t], slots[t]
            if right is not None:
                r, l = r + right, l + left
            right = lax.ppermute(r, 'tp', [(i, i + 1) for i in range(0, min(t, n_tp - 1))])
            left = lax.ppermute(l, 'tp', [(i, i - 1) for i in range(max(n_tp - t, 1), n_tp)])
        return slots[0] + right + left

    def exchange(slots):
        return [slots[0]] + [shift(slots[n_tp - k], n_tp - k) for k in range(1, n_tp)]

    def roll(x, start):
        return lax.dynamic_slice_in_dim(jnp.concatenate([x, x], 0), start, n_tp, 0)

    def device_step(img, txt, vec, ids, d_img, d_txt, w_mod, b_mod, w_qkv, b_qkv, qk_gain, w_proj, b_proj, w_fc1, b_fc1, w_fc2, b_fc2):
        z = lax.axis_index('tp')
        f = lax.axis_index('fsdp')
        batch, length, width = img.shape
        chunks = batch // n_tp
        rows = w_mod.shape[1]
        tokens = (txt, img)
        d_out = (d_txt, d_img)

        silu_vec, silu_pull = jax.vjp(silu_bf16, vec.astype(F32))
        silu_all = lax.all_gather(silu_vec, 'fsdp', axis=0, tiled=True)
        silu_rows = lax.dynamic_slice_in_dim(silu_all, f * rows, rows, 1)
        mod_part = mm('bd,ndke->bnke', silu_rows, w_mod)
        mod_own = lax.psum_scatter(mod_part, 'fsdp', scatter_dimension=0, tiled=True) + b_mod.astype(F32)
        modul = lax.all_gather(mod_own, 'tp', axis=3, tiled=True)

        wq = lax.all_gather(w_qkv, 'fsdp', axis=1, tiled=True)
        proj_slots = jnp.stack(exchange_gather(w_proj, shift, n_tp), 0)
        wp = lax.all_gather(proj_slots, 'fsdp', axis=2, tiled=True)
        w1 = lax.all_gather(w_fc1, 'fsdp', axis=1, tiled=True)
        w2 = lax.all_gather(w_fc2, 'fsdp', axis=1, tiled=True)
        cosine, sine = rope_tables(ids, qk_gain.shape[-1])
        gains = qk_gain.astype(F32)

        def own_sample(x, c):
            return lax.dynamic_index_in_dim(x, n_tp * c + z, 0, keepdims=True)

        state = []
        for c in range(chunks):
            part = slice(n_tp * c, n_tp * (c + 1))
            h1, raw, pulls, joint = [], [], [], ([], [], [])
            for b in range(2):
                h1.append(modulate(tokens[b][part].astype(F32), modul[part, b, 0], modul[part, b, 1]))
                raw.append(mm('bld,dke->blke', h1[b], wq[b]) + b_qkv[b].astype(F32))
                span = slice(b * length, (b + 1) * length)
                prep = functools.partial(qk_prep, cosine=cosine[part, span], sine=sine[part, span])
                prepared, pull = jax.vjp(prep, raw[b], gains[b])
                pulls.append(pull)
                for i in range(3):
                    joint[i].append(prepared[i])
            heads, attn_pull = jax.vjp(attend, *(jnp.concatenate(p, 1) for p in joint))
            flat = heads.reshape(n_tp, 2 * length, -1)
            got = exchange([lax.dynamic_index_in_dim(flat, (z + k) % n_tp, 0, keepdims=False) for k in range(n_tp)])
            attn_own = jnp.stack(got, 1)
            mod_c = own_sample(modul, c)
            s = dict(h1=h1, pulls=pulls, attn_pull=attn_pull, attn_own=attn_own, mod_own=mod_c, heads_shape=heads.shape)
            own, h2_own = [], []
            for b in range(2):
                m = mod_c[:, b]
                a = attn_own[b * length:(b + 1) * length]
                proj = jnp.sum(mm('lgk,gkd->gld', a, wp[:, b]).astype(BF16).astype(F32), 0)[None] + b_proj[b].astype(F32)
                x_own = own_sample(tokens[b], c).astype(F32)
                x1 = x_own + m[:, 2, None, :] * proj
                h2, pull = jax.vjp(modulate, x1, m[:, 3], m[:, 4])
                own.append(dict(proj=proj, x_own=x_own, x1=x1, norm2_pull=pull))
                h2_own.append(h2[0])
            s['own'] = own
            slots = line_gather(jnp.stack(h2_own, 0), z)
            s['h2'] = [jnp.stack([t[b] for t in slots], 0) for b in range(2)]
            state.append(s)

        d_b_fc2 = [0.0, 0.0]
        for c in range(chunks):
            s = state[c]
            part = slice(n_tp * c, n_tp * (c + 1))
            s['d_mlp'], s['hidden'], s['d_pre'], s['d_pre_bf'], mlp_parts, d_h2 = [], [], [], [], [], []
            for b in range(2):
                pre = mm('bld,df->blf', s['h2'][b], w1[b]) + b_fc1[b].astype(F32)
                hidden, gelu_pull = jax.vjp(gelu_bf16, pre)
                mlp_parts.append(mm('blf,fd->bld', hidden, w2[b]).astype(BF16))
                d_mlp = roll(modul[part, b, 5], z)[:, None, :] * roll(d_out[b][part], z).astype(F32)
                d_b_fc2[b] = d_b_fc2[b] + jnp.sum(d_mlp, (0, 1))
                d_mlp_bf = d_mlp.astype(BF16)
                d_hidden = mm('bld,fd->blf', d_mlp_bf, w2[b]).astype(BF16)
                d_pre = gelu_pull(d_hidden)[0]
                d_pre_bf = d_pre.astype(BF16)
                d_h2.append(mm('blf,df->bld', d_pre_bf, w1[b]))
                s['d_mlp'].append(d_mlp_bf)
                s['hidden'].append(hidden)
                s['d_pre'].append(jnp.sum(d_pre, (0, 1)))
                s['d_pre_bf'].append(d_pre_bf)
            s['d_h2'] = line_scatter([jnp.stack([d_h2[b][k] for b in range(2)], 0) for k in range(n_tp)]).astype(BF16)
            s['mlp_parts'] = mlp_parts

        def cat(name, b):
            return jnp.concatenate([s[name][b] for s in state], 0)

        def rows_out(grad_full, axis):
            return lax.psum_scatter(grad_full, 'fsdp', scatter_dimension=axis, tiled=True) * grad_scale

        g_fc2 = [rows_out(mm('blf,bld->fd', cat('hidden', b), cat('d_mlp', b)), 0) for b in range(2)]
        g_fc1 = [rows_out(mm('bld,blf->df', cat('h2', b), cat('d_pre_bf', b)), 0) for b in range(2)]
        d_b_fc1 = [sum(s['d_pre'][b] for s in state) for b in range(2)]

        d_b_proj = [0.0, 0.0]
        for c in range(chunks):
            s = state[c]
            s['d_attn_groups'], s['d_proj'], s['d_resid'], s['tail'] = [], [], [], []
            for b in range(2):
                m = s['mod_own'][:, b]
                o = s['own'][b]
                d_own = own_sample(d_out[b], c).astype(F32)
                d_resid, d_shift2, d_scale2 = o['norm2_pull'](s['d_h2'][b][None])
                d_resid = d_resid + d_own
                d_proj = m[:, 2, None, :] * d_resid
                d_b_proj[b] = d_b_proj[b] + jnp.sum(d_proj, (0, 1))
                d_proj_bf = d_proj.astype(BF16)
                s['d_attn_groups'].append(mm('bld,gkd->glk', d_proj_bf, wp[:, b]).astype(BF16))
                s['d_proj'].append(d_proj_bf)
                s['d_resid'].append(d_resid)
                s['tail'].append((jnp.sum(d_resid * o['proj'], 1), d_shift2, d_scale2))
            groups = jnp.concatenate(s['d_attn_groups'], 1)
            got = exchange([groups[k] for k in range(n_tp)])
            s['d_attn'] = roll(jnp.stack(got, 0), (n_tp - z) % n_tp)
        g_proj = []
        for b in range(2):
            a = jnp.concatenate([s['attn_own'][b * length:(b + 1) * length] for s in state], 0)
            d = jnp.concatenate([s['d_proj'][b][0] for s in state], 0)
            part_sum = lax.psum_scatter(mm('lgk,ld->gkd', a, d), 'fsdp', scatter_dimension=1, tiled=True)
            g_proj.append(line_scatter([part_sum[k] for k in range(n_tp)]) * grad_scale)

        outs = [[], []]
        for c in range(chunks):
            s = state[c]
            got = exchange([jnp.stack([s['mlp_parts'][b][k] for b in range(2)], 0) for k in range(n_tp)])
            total = sum(g.astype(F32) for g in got)
            own_out = []
            for b in range(2):
                m = s['mod_own'][:, b]
                mlp = total[b][None] + b_fc2[b].astype(F32)
                d_own = own_sample(d_out[b], c).astype(F32)
                s['tail'][b] = s['tail'][b] + (jnp.sum(d_own * mlp, 1),)
                own_out.append((s['own'][b]['x1'] + m[:, 5, None, :] * mlp).astype(BF16)[0])
            slots = line_gather(jnp.stack(own_out, 0), z)
            for b in range(2):
                outs[b].append(roll(jnp.stack([t[b] for t in slots], 0), (n_tp - z) % n_tp))

        d_gain = [0.0, 0.0]
        d_b_qkv = [0.0, 0.0]
        for c in range(chunks):
            s = state[c]
            d_joint = s['attn_pull'](s['d_attn'].reshape(s['heads_shape']))
            s['d_raw'], d_h1 = [], []
            for b in range(2):
                span = slice(b * length, (b + 1) * length)
                d_raw, dg = s['pulls'][b](tuple(g[:, span] for g in d_joint))
                d_gain[b] = d_gain[b] + dg
                d_b_qkv[b] = d_b_qkv[b] + jnp.sum(d_raw, (0, 1))
                d_raw_bf = d_raw.astype(BF16)
                s['d_raw'].append(d_raw_bf)
                d_h1.append(mm('blke,dke->bld', d_raw_bf, wq[b]))
            s['d_h1'] = line_scatter([jnp.stack([lax.dynamic_index_in_dim(d_h1[b], (z + k) % n_tp, 0, keepdims=False) for b in range(2)], 0) for k in range(n_tp)]).astype(BF16)
        g_qkv = [rows_out(mm('bld,blke->dke', cat('h1', b), cat('d_raw', b)), 0) for b in range(2)]
        g_tok = [[], []]
        d_mod_own = []
        for c in range(chunks):
            s = state[c]
            own_g, rows_b = [], []
            for b in range(2):
                m = s['mod_own'][:, b]
                _, pull = jax.vjp(modulate, s['own'][b]['x_own'], m[:, 0], m[:, 1])
                d_tokens, d_shift1, d_scale1 = pull(s['d_h1'][b][None])
                own_g.append((d_tokens + s['d_resid'][b]).astype(BF16)[0])
                d_gate1, d_shift2, d_scale2, d_gate2 = s['tail'][b]
                rows_b.append(jnp.concatenate([d_shift1, d_scale1, d_gate1, d_shift2, d_scale2, d_gate2], 0))
            d_mod_own.append(jnp.stack(rows_b, 0))
            slots = line_gather(jnp.stack(own_g, 0), z)
            for b in range(2):
                g_tok[b].append(roll(jnp.stack([t[b] for t in slots], 0), (n_tp - z) % n_tp))

        d_mod = jnp.stack(d_mod_own, 0)
        d_mod = d_mod.reshape(chunks, 2, 6, n_tp, width // n_tp)
        d_cols = lax.all_to_all(d_mod, 'tp', 3, 0, tiled=True).reshape(n_tp, chunks, 2, 6, width // n_tp)
        d_cols = jnp.swapaxes(d_cols, 0, 1).reshape(batch, 2, 6, width // n_tp)
        d_all = lax.all_gather(d_cols.astype(BF16), 'fsdp', axis=0, tiled=True)
        g_mod = mm('bd,bnke->ndke', silu_rows, d_all) * grad_scale
        d_silu = lax.psum(mm('bnke,ndke->bd', d_all, w_mod), 'tp').astype(BF16)
        d_silu = lax.all_to_all(d_silu, 'fsdp', 0, 1, tiled=True)
        g_vec = silu_pull(d_silu)[0]

        g_b_mod, g_b_qkv, g_b_fc1, g_b_fc2 = (v * grad_scale for v in lax.psum((jnp.sum(d_cols, 0), jnp.stack(d_b_qkv), jnp.stack(d_b_fc1), jnp.stack(d_b_fc2)), 'fsdp'))
        g_gain, g_b_proj = (v * grad_scale for v in lax.psum((jnp.stack(d_gain), jnp.stack(d_b_proj)), ('tp', 'fsdp')))
        full = [jnp.concatenate(outs[b], 0) for b in range(2)]
        g_full = [jnp.concatenate(g_tok[b], 0) for b in range(2)]
        return (full[1], full[0], g_full[1], g_full[0], g_vec, g_mod, g_b_mod, jnp.stack(g_qkv), g_b_qkv, g_gain, jnp.concatenate([g[None] if g.ndim == 2 else g for g in g_proj], 0), g_b_proj, jnp.stack(g_fc1), g_b_fc1, jnp.stack(g_fc2), g_b_fc2)

    return jax.shard_map(device_step, mesh=mesh, in_specs=in_specs, out_specs=out_specs, check_vma=False)


def exchange_gather(own, shift, n_tp):
    return [own] + [shift(own, n_tp - k) for k in range(1, n_tp)]
```
